32 devices in a mesh: node: 16 (over z, y, core), local: 2 (over x).
Axes of the slice: x: 2, y: 2, z: 4, core: 2. Of those that a mesh axis runs over, the one named last changes fastest.
Arguments:
- tokens: bfloat16 [5120, 4096], P(('node', 'local')), may hold values from -6 to 6
- out_grad: bfloat16 [5120, 4096], P(('node', 'local')), may hold values from -6 to 6
- up_codes: bfloat16 [4096, 256], P('local'), may hold values from -127 to 127
- up_scales: float32 [4096, 2], P('local'), may hold values from 0.000109375 to 0.0004375
- down_codes: bfloat16 [4096, 256], P('local'), may hold values from -127 to 127
- down_scales: float32 [4096, 2], P('local'), may hold values from 0.000109375 to 0.0004375
Outputs:
- input_grad: bfloat16 [5120, 4096], P(('node', 'local'))
- grad_up: float32 [4096, 256], P(('local', 'node'))
- grad_down: float32 [4096, 256], P(('local', 'node'))
The draws below stay inside these ranges and needn't reach their ends.
All inputs are finite; a program needn't handle non-finite values.
Results may differ from the reference program's by a relative error of at most 0.0075.
Values sent between devices are 32-bit elements; how exact they have to be, the bound alone decides.
A program may use at most 128 MiB of HBM per device.

```python
import math
import jax
import jax.numpy as jnp
from jax import lax

D = 4096
BUCKET = 256
QBLOCK = 128
TOK_DEV = 160
NBLOCK = 2
TOKENS = 5120
N_NODE = 16
N_LOCAL = 2


def with_spikes(values, key, source, target, parts, factor):
    owner, partner = [(jnp.arange(values.shape[dim]) // (values.shape[dim] // parts)).reshape([-1 if axis == dim else 1 for axis in range(values.ndim)]) for dim in (source, target)]
    chosen = jax.random.permutation(key, parts)[partner]
    strong = (owner == chosen) | (owner == (partner + parts // 2) % parts)
    return jnp.where(strong, factor * values, values)


def levels(stream_key, shape, pieces, low, largest):
    gain, own = 1.0, jax.random.fold_in(stream_key, 6)
    for axis_at, parts in pieces:
        steps = jnp.exp(jax.random.uniform(jax.random.fold_in(own, axis_at), (parts,), jnp.float32, low / len(pieces), largest / len(pieces)))
        gain = gain * jnp.repeat(steps, shape[axis_at] // parts).reshape([-1 if axis == axis_at else 1 for axis in range(len(shape))])
    return gain


def bell_draw_with(own_key, extent, spread, limit, pieces, heavy, kind=jnp.bfloat16):
    result = spread * jax.random.normal(own_key, extent, jnp.float32)
    if pieces:
        result = result * levels(own_key, extent, pieces, -0.22, 0.18)
    return jnp.clip(with_spikes(result, jax.random.fold_in(own_key, 3), *heavy), -limit, limit).astype(kind)


def setup_inputs(seed: int = 0) -> dict:
    seeds = jax.random.split(jax.random.key(seed), 7)
    tokens = bell_draw_with(seeds[0], (TOKENS, D), 1.0, 6.0, ((0, 32),), (0, 1, 32, 2.75))
    out_grad = bell_draw_with(seeds[1], (TOKENS, D), 1.0, 6.0, ((0, 32),), (0, 1, 32, 2.75))
    up_codes = jnp.clip(jax.random.uniform(seeds[2], (D, BUCKET), jnp.float32, -127.0, 127.0) * levels(seeds[2], (D, BUCKET), ((0, 2),), -0.4, 0.0), -127.0, 127.0).astype(jnp.bfloat16)
    up_scales = jnp.clip(jnp.exp(math.log(0.0004375) - 1.3862944 * jax.random.uniform(seeds[3], (D, NBLOCK), jnp.float32) ** levels(seeds[3], (D, NBLOCK), ((0, 2),), -0.2, 0.2)), 0.000109375, 0.0004375)
    down_codes = jnp.clip(jax.random.uniform(seeds[4], (D, BUCKET), jnp.float32, -127.0, 127.0) * levels(seeds[4], (D, BUCKET), ((0, 2),), -0.4, 0.0), -127.0, 127.0).astype(jnp.bfloat16)
    down_scales = jnp.clip(jnp.exp(math.log(0.0004375) - 1.3862944 * jax.random.uniform(seeds[5], (D, NBLOCK), jnp.float32) ** levels(seeds[5], (D, NBLOCK), ((0, 2),), -0.2, 0.2)), 0.000109375, 0.0004375)
    return {"tokens": tokens, "out_grad": out_grad, "up_codes": up_codes, "up_scales": up_scales, "down_codes": down_codes, "down_scales": down_scales}


def gelu_tanh(values):
    return jax.nn.gelu(values, approximate=True)

def quantize(values):
    blocks = values.reshape(values.shape[:-1] + (values.shape[-1] // QBLOCK, QBLOCK))
    scales = 2.0 * jnp.sqrt(lax.optimization_barrier(jnp.mean(blocks * blocks, axis=-1)) + 1e-06) / 7.0
    block_codes = jnp.clip(blocks / scales[..., None], -7.0, 7.0).astype(jnp.bfloat16).reshape(values.shape)
    return (block_codes, scales)

def restore(block_codes, scales):
    blocks = block_codes.astype(jnp.float32).reshape(block_codes.shape[:-1] + (scales.shape[-1], -1))
    return (blocks * scales[..., None]).reshape(block_codes.shape)

def reference(tokens, out_grad, up_codes, up_scales, down_codes, down_scales):
    up = restore(up_codes, up_scales).astype(jnp.bfloat16)
    down = restore(down_codes, down_scales).astype(jnp.bfloat16)
    preact = jnp.dot(tokens, up, preferred_element_type=jnp.float32)
    activated, slope_fn = jax.vjp(gelu_tanh, preact)
    activated = activated.astype(jnp.bfloat16)
    back_grad = jnp.dot(out_grad, down, preferred_element_type=jnp.float32)
    hidden_grad = slope_fn(back_grad)[0].astype(jnp.bfloat16)
    input_grad = jnp.dot(hidden_grad, up.T, preferred_element_type=jnp.float32).astype(jnp.bfloat16)
    token_blocks = tokens.reshape(N_NODE, N_LOCAL, TOK_DEV, D)
    out_blocks = out_grad.reshape(N_NODE, N_LOCAL, TOK_DEV, D)
    hidden_blocks = hidden_grad.reshape(N_NODE, N_LOCAL, TOK_DEV, BUCKET)
    active_blocks = activated.reshape(N_NODE, N_LOCAL, TOK_DEV, BUCKET)

    def device_term(inner):
        inputs, outs, hiddens, actives = inner
        first = jnp.dot(inputs.T, hiddens, preferred_element_type=jnp.float32)
        second = jnp.dot(outs.T, actives, preferred_element_type=jnp.float32)
        block_codes, scales = quantize(jnp.stack([first, second]))
        return restore(block_codes, scales)

    def node_step(carry, node_items):
        summed = lax.optimization_barrier(jnp.sum(lax.map(device_term, node_items), axis=0))
        block_codes, scales = quantize(summed)
        return (carry + restore(block_codes, scales), None)
    total, _ = lax.scan(node_step, jnp.zeros((2, D, BUCKET), jnp.float32), (token_blocks, out_blocks, hidden_blocks, active_blocks))
    total = total / (N_NODE * N_LOCAL)
    return (input_grad, total[0], total[1])
```

```python
import functools

import jax
import jax.numpy as jnp
from jax import lax
from jax.experimental import pallas as pl
from jax.experimental.pallas import tpu as pltpu
from jax.sharding import PartitionSpec as P

QBLOCK = 128
MESH = pl.DeviceIdType.MESH
F32 = jnp.float32
BF16 = jnp.bfloat16


def restored(block_codes, scales):
    blocks = block_codes.astype(F32).reshape(block_codes.shape[:-1] + (scales.shape[-1], -1))
    return (blocks * scales[..., None]).reshape(block_codes.shape)


def coded(values, axis):
    power = jnp.mean(values * values, axis=axis, keepdims=True) + 1e-06
    inverse = lax.rsqrt(power)
    scale = (2.0 / 7.0) * (power * inverse)
    codes = jnp.clip(values * (3.5 * inverse), -7.0, 7.0).astype(BF16).astype(F32)
    return codes * scale


def place(index, order):
    return sum(((index // (1 << bit)) % 2) * (1 << at) for at, bit in enumerate(order))


def flipped(index, bit):
    return index + (1 - 2 * ((index // (1 << bit)) % 2)) * (1 << bit)


def kernel(
    n_node, n_local, pieces, early,
    tok, og, up, dn, own_slice, ig, gu, gd,
    xs, xr, wb, wide, hid, act, hs, hr, g, r,
    x_send, x_recv, w_send, w_recv, a_send, a_recv, h_send, h_recv, r_send, r_recv,
):
    node, loc = lax.axis_index("node"), lax.axis_index("local")
    tokens, depth = tok.shape
    hidden = up.shape[1]
    rows = depth // n_local
    owned = rows // n_node
    bits = n_node.bit_length() - 1
    flip_layout = owned % 128 == 0
    others = range(1, n_local)
    halves = hidden // QBLOCK
    piece = tokens // pieces

    def target(step):
        return lax.rem(loc + step, n_local)

    def source(step):
        return lax.rem(loc + n_local - step, n_local)

    def columns(index):
        return pl.ds(pl.multiple_of(index * rows, 128), rows)

    barrier = pltpu.get_barrier_semaphore()
    for step in others:
        pl.semaphore_signal(barrier, inc=1, device_id={"local": target(step)}, device_id_type=MESH)
    for bit in range(bits):
        pl.semaphore_signal(barrier, inc=1, device_id={"node": flipped(node, bit)}, device_id_type=MESH)
    pl.semaphore_wait(barrier, n_local - 1 + bits)

    far = [bit for bit in range(bits - 1, -1, -1)]
    near = [1] + [bit for bit in range(bits - 1, 1, -1)] + [0] if bits > 1 else far
    gather_orders = (far, near)

    w_copies = {}
    for m in range(2):
        for step in others:
            w_copies[m, step] = pltpu.make_async_remote_copy(
                src_ref=own_slice.at[m],
                dst_ref=wb.at[step - 1, m, place(node, gather_orders[m])],
                send_sem=w_send.at[step - 1, m],
                recv_sem=w_recv.at[step - 1, m],
                device_id={"local": target(step)},
                device_id_type=MESH,
            )
            w_copies[m, step].start()

    x_copies = {}
    for m in range(2):
        for step in others:
            xs[step - 1, m] = (tok, og)[m][:, columns(target(step))].astype(F32)
            for c in range(pieces):
                x_copies[m, step, c] = pltpu.make_async_remote_copy(
                    src_ref=xs.at[step - 1, m, pl.ds(c * piece, piece)],
                    dst_ref=xr.at[step - 1, m, pl.ds(c * piece, piece)],
                    send_sem=x_send.at[step - 1, m, c],
                    recv_sem=x_recv.at[step - 1, m, c],
                    device_id={"local": target(step)},
                    device_id_type=MESH,
                )
                if m == 0 or c < early:
                    x_copies[m, step, c].start()

    sums = [
        jnp.dot(tok[:, columns(loc)], up[...], preferred_element_type=F32),
        jnp.dot(og[:, columns(loc)], dn[...], preferred_element_type=F32),
    ]

    a_copies = {}
    for stage in range(bits):
        for m in range(2):
            for step in others:
                if stage == 0:
                    w_copies[m, step].wait_recv()
                else:
                    a_copies[m, step, stage - 1].wait_recv()
                size = 1 << stage
                at = place(node, gather_orders[m])
                held = wb.at[step - 1, m, pl.ds((at // size) * size, size)]
                a_copies[m, step, stage] = pltpu.make_async_remote_copy(
                    src_ref=held,
                    dst_ref=held,
                    send_sem=a_send.at[step - 1, m, stage],
                    recv_sem=a_recv.at[step - 1, m, stage],
                    device_id={"node": flipped(node, gather_orders[m][stage])},
                    device_id_type=MESH,
                )
                a_copies[m, step, stage].start()
    for m in range(2):
        for step in others:
            a_copies[m, step, bits - 1].wait_recv()
            for n in range(n_node):
                wide[step - 1, m, n * owned : (n + 1) * owned, :] = wb[
                    step - 1, m, place(n, gather_orders[m])
                ].astype(BF16)
            sums[m] += jnp.dot(
                (tok, og)[m][:, columns(source(step))],
                wide[step - 1, m],
                preferred_element_type=F32,
            )

    pre, back = sums
    root = 0.7978845608028654
    square = pre * pre
    bend = jnp.tanh(root * (pre + 0.044715 * (square * pre)))
    half = 0.5 * (1.0 + bend)
    slope = half + 0.5 * pre * (1.0 - bend * bend) * (root * (1.0 + 3.0 * 0.044715 * square))
    act[...] = (half * pre).astype(BF16)
    hid[...] = (back * slope).astype(BF16)
    hs[0] = hid[...].astype(F32)
    hs[1] = act[...].astype(F32)
    h_copies = {}
    for m in range(2):
        for step in others:
            h_copies[m, step] = pltpu.make_async_remote_copy(
                src_ref=hs.at[m],
                dst_ref=hr.at[step - 1, m],
                send_sem=h_send.at[step - 1, m],
                recv_sem=h_recv.at[step - 1, m],
                device_id={"local": target(step)},
                device_id_type=MESH,
            )
            h_copies[m, step].start()
    for c in range(early, pieces):
        for step in others:
            x_copies[1, step, c].start()

    across = (((1,), (1,)), ((), ()))
    ig[:, columns(loc)] = lax.dot_general(
        hid[...], up[...], across, preferred_element_type=F32
    ).astype(BF16)
    for step in others:
        ig[:, columns(source(step))] = lax.dot_general(
            hid[...], wide[step - 1, 0], across, preferred_element_type=F32
        ).astype(BF16)

    chunks = [(m, f) for m in range(2) for f in range(halves)]
    add_orders = [gather_orders[k % 2] for k in range(len(chunks))]
    down_rows = (((0,), (0,)), ((), ()))
    axis = 0 if flip_layout else 1
    block = max(owned, min(rows, 256))

    def term(features, values):
        pair = (features, values) if flip_layout else (values, features)
        return coded(lax.dot_general(*pair, down_rows, preferred_element_type=F32), axis)

    def compute(k):
        m, f = chunks[k]
        lanes = slice(f * QBLOCK, (f + 1) * QBLOCK)
        if f == 0:
            for step in others:
                h_copies[m, step].wait_recv()
                for c in range(pieces):
                    x_copies[m, step, c].wait_recv()
        mine = (hid, act)[m][:, lanes]
        theirs = [hr[step - 1, m, :, lanes].astype(BF16) for step in others]
        for start in range(0, rows, block):
            own = (tok, og)[m][:, pl.ds(pl.multiple_of(loc * rows + start, 128), block)]
            total = term(mine, own)
            for step in others:
                total += term(
                    theirs[step - 1], xr[step - 1, m, :, start : start + block].astype(BF16)
                )
            total = coded(total, axis)
            for sub in range(block // owned):
                at = place(start // owned + sub, add_orders[k])
                cut = slice(sub * owned, (sub + 1) * owned)
                g[k, at] = total[:, cut] if flip_layout else total[cut, :]

    region = [0] * len(chunks)
    r_copies = {}

    def start(k, stage):
        bit = add_orders[k][bits - 1 - stage]
        size = n_node >> (stage + 1)
        mine = (node // (1 << bit)) % 2
        r_copies[k, stage] = pltpu.make_async_remote_copy(
            src_ref=g.at[k, pl.ds(region[k] + (1 - mine) * size, size)],
            dst_ref=r.at[k, pl.ds(n_node - 2 * size, size)],
            send_sem=r_send.at[k, stage],
            recv_sem=r_recv.at[k, stage],
            device_id={"node": flipped(node, bit)},
            device_id_type=MESH,
        )
        r_copies[k, stage].start()
        region[k] = region[k] + mine * size

    def finish(k, stage):
        size = n_node >> (stage + 1)
        r_copies[k, stage].wait_recv()

        def add(i, carry):
            g[k, region[k] + i] += r[k, n_node - 2 * size + i]
            return carry

        lax.fori_loop(0, size, add, 0)

    def emit(k):
        m, f = chunks[k]
        value = g[k, region[k]] * (1.0 / (n_node * n_local))
        (gu, gd)[m][:, f * QBLOCK : (f + 1) * QBLOCK] = value.T if flip_layout else value

    for tick in range(len(chunks) + bits):
        for k in range(min(tick, len(chunks) - 1), -1, -1):
            stage = tick - k
            if stage > bits:
                continue
            if stage == 0:
                compute(k)
            else:
                finish(k, stage - 1)
            if stage < bits:
                start(k, stage)
            else:
                emit(k)

    for copies in (w_copies, x_copies, a_copies, h_copies, r_copies):
        for copy in copies.values():
            copy.wait_send()


def local(n_node, n_local, tokens, out_grad, up_codes, up_scales, down_codes, down_scales):
    count, depth = tokens.shape
    rows, hidden = up_codes.shape
    owned = rows // n_node
    bits = n_node.bit_length() - 1
    pieces = 4 if count % 32 == 0 else 1
    chunks = 2 * (hidden // QBLOCK)
    others = n_local - 1
    block = (QBLOCK, owned) if owned % 128 == 0 else (owned, QBLOCK)
    up = restored(up_codes, up_scales).astype(BF16)
    down = restored(down_codes, down_scales).astype(BF16)
    at = lax.axis_index("node") * owned
    own_slice = jnp.stack(
        [lax.dynamic_slice_in_dim(w, at, owned, 0).astype(F32) for w in (up, down)]
    )
    dma = pltpu.SemaphoreType.DMA
    vmem = pl.BlockSpec(memory_space=pltpu.VMEM)
    return pl.pallas_call(
        functools.partial(kernel, n_node, n_local, pieces, pieces // 2),
        out_shape=(
            jax.ShapeDtypeStruct((count, depth), BF16),
            jax.ShapeDtypeStruct((owned, hidden), F32),
            jax.ShapeDtypeStruct((owned, hidden), F32),
        ),
        in_specs=[vmem] * 5,
        out_specs=(vmem, vmem, vmem),
        scratch_shapes=[
            pltpu.VMEM((others, 2, count, rows), F32),
            pltpu.VMEM((others, 2, count, rows), F32),
            pltpu.VMEM((others, 2, n_node, owned, hidden), F32),
            pltpu.VMEM((others, 2, rows, hidden), BF16),
            pltpu.VMEM((count, hidden), BF16),
            pltpu.VMEM((count, hidden), BF16),
            pltpu.VMEM((2, count, hidden), F32),
            pltpu.VMEM((others, 2, count, hidden), F32),
            pltpu.VMEM((chunks, n_node) + block, F32),
            pltpu.VMEM((chunks, n_node) + block, F32),
            dma((others, 2, pieces)),
            dma((others, 2, pieces)),
            dma((others, 2)),
            dma((others, 2)),
            dma((others, 2, bits)),
            dma((others, 2, bits)),
            dma((others, 2)),
            dma((others, 2)),
            dma((chunks, bits)),
            dma((chunks, bits)),
        ],
        compiler_params=pltpu.CompilerParams(
            collective_id=0, has_side_effects=True, vmem_limit_bytes=56 * 1024 * 1024
        ),
    )(tokens, out_grad, up, down, own_slice)


def solution(mesh):
    placed = (
        P(("node", "local"), None),
        P(("node", "local"), None),
        P("local", None),
        P("local", None),
        P("local", None),
        P("local", None),
    )
    return jax.shard_map(
        functools.partial(local, mesh.shape["node"], mesh.shape["local"]),
        mesh=mesh,
        in_specs=placed,
        out_specs=(
            P(("node", "local"), None),
            P(("local", "node"), None),
            P(("local", "node"), None),
        ),
        check_vma=False,
    )
```

```python
import functools

import jax
import jax.numpy as jnp
from jax import lax
from jax.experimental import pallas as pl
from jax.experimental.pallas import tpu as pltpu
from jax.sharding import PartitionSpec as P

QBLOCK = 128
MESH = pl.DeviceIdType.MESH
F32 = jnp.float32
BF16 = jnp.bfloat16


def coded(values, axis):
    power = jnp.mean(values * values, axis=axis, keepdims=True) + 1e-06
    inverse = lax.rsqrt(power)
    scale = (2.0 / 7.0) * (power * inverse)
    codes = jnp.clip(values * (3.5 * inverse), -7.0, 7.0).astype(BF16).astype(F32)
    return codes * scale


def paired(first, second):
    left = lax.broadcasted_iota(jnp.int32, first.shape, 1) < QBLOCK // 2
    turn = QBLOCK // 2
    return (
        jnp.where(left, first, pltpu.roll(second, turn, 1)),
        jnp.where(left, pltpu.roll(first, turn, 1), second),
    )


def place(index, order):
    return sum(((index // (1 << bit)) % 2) * (1 << at) for at, bit in enumerate(order))


def flipped(index, bit):
    return index + (1 - 2 * ((index // (1 << bit)) % 2)) * (1 << bit)


def kernel(
    n_node, n_local, paired_rows, pieces,
    tok, og, up_codes, up_scales, dn_codes, dn_scales, ig, gu, gd,
    xs, xr, xo, wf, wn, wb, wide, hid, act, hs, hr, g, r,
    x_send, x_recv, w_send, w_recv, a_send, a_recv, h_send, h_recv, r_send, r_recv,
):
    node, loc = lax.axis_index("node"), lax.axis_index("local")
    tokens, depth = tok.shape
    hidden = up_codes.shape[1]
    up, dn = wn.at[0], wn.at[1]
    rows = depth // n_local
    owned = rows // n_node
    bits = n_node.bit_length() - 1
    parts = 2 if paired_rows else 1
    others = range(1, n_local)
    halves = hidden // QBLOCK
    piece = tokens // pieces

    def target(step):
        return lax.rem(loc + step, n_local)

    def source(step):
        return lax.rem(loc + n_local - step, n_local)

    def columns(index):
        return pl.ds(pl.multiple_of(index * rows, 128), rows)

    barrier = pltpu.get_barrier_semaphore()
    for step in others:
        pl.semaphore_signal(barrier, inc=1, device_id={"local": target(step)}, device_id_type=MESH)
    for bit in range(bits):
        pl.semaphore_signal(barrier, inc=1, device_id={"node": flipped(node, bit)}, device_id_type=MESH)
    pl.semaphore_wait(barrier, n_local - 1 + bits)

    far = [bit for bit in range(bits - 1, -1, -1)]
    near = [1] + [bit for bit in range(bits - 1, 1, -1)] + [0] if bits > 1 else far
    gather_orders = (far, near)

    def stage_columns(values, m, index, store):
        if not paired_rows:
            store(0, slice(0, rows), values[:, columns(index)].astype(F32))
            return
        for pair in range(n_node // 2):
            begin = index * rows + pair * 2 * owned
            both = values[:, pl.ds(pl.multiple_of(begin, 128), 2 * owned)].astype(F32)
            cut = slice(pair * owned, (pair + 1) * owned)
            for part, tile in enumerate(paired(both[:, :owned], both[:, owned:])):
                store(part, cut, tile)

    x_copies = {}
    for m in range(2):
        for step in others:
            for part in range(parts):
                for c in range(pieces):
                    x_copies[m, step, part, c] = pltpu.make_async_remote_copy(
                        src_ref=xs.at[step - 1, m, part, pl.ds(c * piece, piece)],
                        dst_ref=xr.at[step - 1, m, part, pl.ds(c * piece, piece)],
                        send_sem=x_send.at[step - 1, m, part, c],
                        recv_sem=x_recv.at[step - 1, m, part, c],
                        device_id={"local": target(step)},
                        device_id_type=MESH,
                    )

    def send_columns(m, part, c):
        for step in others:
            x_copies[m, step, part, c].start()

    def stage_sends(m):
        for step in others:

            def store(part, cut, tile):
                xs[step - 1, m, part, :, cut] = tile

            stage_columns((tok, og)[m], m, target(step), store)

    stage_sends(0)
    send_columns(0, 0, 0)

    for m, (codes, scales) in enumerate(((up_codes, up_scales), (dn_codes, dn_scales))):
        for begin in range(0, rows, QBLOCK):
            down_cut = slice(begin, begin + QBLOCK)
            for f in range(halves):
                lanes = slice(f * QBLOCK, (f + 1) * QBLOCK)
                wide_scales = jnp.broadcast_to(scales[f : f + 1, down_cut], (QBLOCK, QBLOCK)).T
                value = (codes[down_cut, lanes].astype(F32) * wide_scales).astype(BF16)
                wn[m, down_cut, lanes] = value
                wf[m, down_cut, lanes] = value.astype(F32)

    w_copies = {}
    for m in range(2):
        for step in others:
            w_copies[m, step] = pltpu.make_async_remote_copy(
                src_ref=wf.at[m, pl.ds(pl.multiple_of(node * owned, 8), owned)],
                dst_ref=wb.at[step - 1, m, place(node, gather_orders[m])],
                send_sem=w_send.at[step - 1, m],
                recv_sem=w_recv.at[step - 1, m],
                device_id={"local": target(step)},
                device_id_type=MESH,
            )
            w_copies[m, step].start()

    queue = [(m, part, c) for m in range(2) for part in range(parts) for c in range(pieces)][1:]
    early = len(queue) - len(queue) // 2
    for m, part, c in queue[:early]:
        if m == 0:
            send_columns(m, part, c)
    stage_sends(1)
    for m, part, c in queue[:early]:
        if m == 1:
            send_columns(m, part, c)
    if paired_rows:
        for m in range(2):

            def keep(part, cut, tile):
                xo[m, part, :, cut] = tile.astype(BF16)

            stage_columns((tok, og)[m], m, loc, keep)

    sums = [
        jnp.dot(tok[:, columns(loc)], up[...], preferred_element_type=F32),
        jnp.dot(og[:, columns(loc)], dn[...], preferred_element_type=F32),
    ]

    a_copies = {}
    for stage in range(bits):
        for m in range(2):
            for step in others:
                if stage == 0:
                    w_copies[m, step].wait_recv()
                else:
                    a_copies[m, step, stage - 1].wait_recv()
                size = 1 << stage
                at = place(node, gather_orders[m])
                held = wb.at[step - 1, m, pl.ds((at // size) * size, size)]
                a_copies[m, step, stage] = pltpu.make_async_remote_copy(
                    src_ref=held,
                    dst_ref=held,
                    send_sem=a_send.at[step - 1, m, stage],
                    recv_sem=a_recv.at[step - 1, m, stage],
                    device_id={"node": flipped(node, gather_orders[m][stage])},
                    device_id_type=MESH,
                )
                a_copies[m, step, stage].start()
    for m in range(2):
        for step in others:
            a_copies[m, step, bits - 1].wait_recv()
            for n in range(n_node):
                wide[step - 1, m, n * owned : (n + 1) * owned, :] = wb[
                    step - 1, m, place(n, gather_orders[m])
                ].astype(BF16)
            sums[m] += jnp.dot(
                (tok, og)[m][:, columns(source(step))],
                wide[step - 1, m],
                preferred_element_type=F32,
            )

    pre, back = sums
    root = 0.7978845608028654
    square = pre * pre
    bend = jnp.tanh(root * (pre + 0.044715 * (square * pre)))
    half = 0.5 * (1.0 + bend)
    slope = half + 0.5 * pre * (1.0 - bend * bend) * (root * (1.0 + 3.0 * 0.044715 * square))
    act[...] = (half * pre).astype(BF16)
    hid[...] = (back * slope).astype(BF16)
    hs[0] = hid[...].astype(F32)
    hs[1] = act[...].astype(F32)
    h_copies = {}
    for m in range(2):
        for step in others:
            h_copies[m, step] = pltpu.make_async_remote_copy(
                src_ref=hs.at[m],
                dst_ref=hr.at[step - 1, m],
                send_sem=h_send.at[step - 1, m],
                recv_sem=h_recv.at[step - 1, m],
                device_id={"local": target(step)},
                device_id_type=MESH,
            )
            h_copies[m, step].start()
    for m, part, c in queue[early:]:
        send_columns(m, part, c)

    across = (((1,), (1,)), ((), ()))
    ig[:, columns(loc)] = lax.dot_general(
        hid[...], up[...], across, preferred_element_type=F32
    ).astype(BF16)
    for step in others:
        ig[:, columns(source(step))] = lax.dot_general(
            hid[...], wide[step - 1, 0], across, preferred_element_type=F32
        ).astype(BF16)

    chunks = [(m, f) for m in range(2) for f in range(2 if paired_rows else halves)]
    add_orders = [gather_orders[k % 2] for k in range(len(chunks))]
    down_rows = (((0,), (0,)), ((), ()))
    axis = 0 if paired_rows else 1
    width = rows // parts
    block = min(width, 256)

    def term(features, values):
        pair = (features, values) if paired_rows else (values, features)
        return coded(lax.dot_general(*pair, down_rows, preferred_element_type=F32), axis)

    def compute(k):
        m, f = chunks[k]
        part = f if paired_rows else 0
        for step in others:
            if f == 0:
                h_copies[m, step].wait_recv()
            if paired_rows or f == 0:
                for c in range(pieces):
                    x_copies[m, step, part, c].wait_recv()
        for start in range(0, width, block):
            cut = slice(start, start + block)
            if paired_rows:
                own = xo[m, part, :, cut]
            else:
                own = (tok, og)[m][:, pl.ds(pl.multiple_of(loc * rows + start, 128), block)]
            received = [xr[step - 1, m, part, :, cut].astype(BF16) for step in others]
            totals = []
            for at in range(halves) if paired_rows else (f,):
                lanes = slice(at * QBLOCK, (at + 1) * QBLOCK)
                total = term((hid, act)[m][:, lanes], own)
                for step in others:
                    total += term(hr[step - 1, m, :, lanes].astype(BF16), received[step - 1])
                totals.append(coded(total, axis))
            if paired_rows:
                for tile in range(block // QBLOCK):
                    lanes = slice(tile * QBLOCK, (tile + 1) * QBLOCK)
                    owner = 2 * (start // QBLOCK + tile)
                    for sub, value in enumerate(paired(totals[0][:, lanes], totals[1][:, lanes])):
                        g[k, place(owner + sub, add_orders[k])] = value
            else:
                for sub in range(block // owned):
                    at = place(start // owned + sub, add_orders[k])
                    g[k, at] = totals[0][sub * owned : (sub + 1) * owned, :]

    region = [0] * len(chunks)
    r_copies = {}

    def start(k, stage):
        bit = add_orders[k][bits - 1 - stage]
        size = n_node >> (stage + 1)
        mine = (node // (1 << bit)) % 2
        r_copies[k, stage] = pltpu.make_async_remote_copy(
            src_ref=g.at[k, pl.ds(region[k] + (1 - mine) * size, size)],
            dst_ref=r.at[k, pl.ds(n_node - 2 * size, size)],
            send_sem=r_send.at[k, stage],
            recv_sem=r_recv.at[k, stage],
            device_id={"node": flipped(node, bit)},
            device_id_type=MESH,
        )
        r_copies[k, stage].start()
        region[k] = region[k] + mine * size

    def finish(k, stage):
        size = n_node >> (stage + 1)
        r_copies[k, stage].wait_recv()

        def add(i, carry):
            g[k, region[k] + i] += r[k, n_node - 2 * size + i]
            return carry

        lax.fori_loop(0, size, add, 0)

    def emit(k):
        m, f = chunks[k]
        value = g[k, region[k]] * (1.0 / (n_node * n_local))
        if paired_rows:
            turned = value.T
            size = owned // 2
            for at in range(2):
                (gu, gd)[m][f * size : (f + 1) * size, at * QBLOCK : (at + 1) * QBLOCK] = turned[
                    at * size : (at + 1) * size
                ]
        else:
            (gu, gd)[m][:, f * QBLOCK : (f + 1) * QBLOCK] = value

    for tick in range(len(chunks) + bits):
        for k in range(min(tick, len(chunks) - 1), -1, -1):
            stage = tick - k
            if stage > bits:
                continue
            if stage == 0:
                compute(k)
            else:
                finish(k, stage - 1)
            if stage < bits:
                start(k, stage)
            else:
                emit(k)

    for copies in (w_copies, x_copies, a_copies, h_copies, r_copies):
        for copy in copies.values():
            copy.wait_send()


def local(n_node, n_local, tokens, out_grad, up_codes, up_scales, down_codes, down_scales):
    count, depth = tokens.shape
    rows, hidden = up_codes.shape
    owned = rows // n_node
    bits = n_node.bit_length() - 1
    pieces = 2 if count % 16 == 0 else 1
    paired_rows = owned == QBLOCK and hidden == 2 * QBLOCK and n_node % 2 == 0
    parts = 2 if paired_rows else 1
    chunks = 4 if paired_rows else 2 * (hidden // QBLOCK)
    others = n_local - 1
    block = (owned, QBLOCK)
    dma = pltpu.SemaphoreType.DMA
    vmem = pl.BlockSpec(memory_space=pltpu.VMEM)
    return pl.pallas_call(
        functools.partial(kernel, n_node, n_local, paired_rows, pieces),
        out_shape=(
            jax.ShapeDtypeStruct((count, depth), BF16),
            jax.ShapeDtypeStruct((owned, hidden), F32),
            jax.ShapeDtypeStruct((owned, hidden), F32),
        ),
        in_specs=[vmem] * 6,
        out_specs=(vmem, vmem, vmem),
        scratch_shapes=[
            pltpu.VMEM((others, 2, parts, count, rows // parts), F32),
            pltpu.VMEM((others, 2, parts, count, rows // parts), F32),
            pltpu.VMEM((2, parts, count, rows // parts), BF16),
            pltpu.VMEM((2, rows, hidden), F32),
            pltpu.VMEM((2, rows, hidden), BF16),
            pltpu.VMEM((others, 2, n_node, owned, hidden), F32),
            pltpu.VMEM((others, 2, rows, hidden), BF16),
            pltpu.VMEM((count, hidden), BF16),
            pltpu.VMEM((count, hidden), BF16),
            pltpu.VMEM((2, count, hidden), F32),
            pltpu.VMEM((others, 2, count, hidden), F32),
            pltpu.VMEM((chunks, n_node) + block, F32),
            pltpu.VMEM((chunks, n_node) + block, F32),
            dma((others, 2, parts, pieces)),
            dma((others, 2, parts, pieces)),
            dma((others, 2)),
            dma((others, 2)),
            dma((others, 2, bits)),
            dma((others, 2, bits)),
            dma((others, 2)),
            dma((others, 2)),
            dma((chunks, bits)),
            dma((chunks, bits)),
        ],
        compiler_params=pltpu.CompilerParams(
            collective_id=0, has_side_effects=True, vmem_limit_bytes=56 * 1024 * 1024
        ),
    )(tokens, out_grad, up_codes, up_scales.T, down_codes, down_scales.T)


def solution(mesh):
    placed = (
        P(("node", "local"), None),
        P(("node", "local"), None),
        P("local", None),
        P("local", None),
        P("local", None),
        P("local", None),
    )
    return jax.shard_map(
        functools.partial(local, mesh.shape["node"], mesh.shape["local"]),
        mesh=mesh,
        in_specs=placed,
        out_specs=(
            P(("node", "local"), None),
            P(("local", "node"), None),
            P(("local", "node"), None),
        ),
        check_vma=False,
    )
```

```python
import functools

import jax
import jax.numpy as jnp
from jax import lax
from jax.experimental import pallas as pl
from jax.experimental.pallas import tpu as pltpu
from jax.sharding import PartitionSpec as P

QBLOCK = 128
MESH = pl.DeviceIdType.MESH
F32 = jnp.float32
BF16 = jnp.bfloat16


def coded(values, axis):
    power = jnp.mean(values * values, axis=axis, keepdims=True) + 1e-06
    inverse = lax.rsqrt(power)
    scale = (2.0 / 7.0) * (power * inverse)
    codes = jnp.clip(values * (3.5 * inverse), -7.0, 7.0).astype(BF16).astype(F32)
    return codes * scale


def paired(first, second):
    left = lax.broadcasted_iota(jnp.int32, first.shape, 1) < QBLOCK // 2
    turn = QBLOCK // 2
    return (
        jnp.where(left, first, pltpu.roll(second, turn, 1)),
        jnp.where(left, pltpu.roll(first, turn, 1), second),
    )


def place(index, order):
    return sum(((index // (1 << bit)) % 2) * (1 << at) for at, bit in enumerate(order))


def flipped(index, bit):
    return index + (1 - 2 * ((index // (1 << bit)) % 2)) * (1 << bit)


def kernel(
    n_node, n_local, paired_rows, pieces,
    tok, og, up_codes, up_scales, dn_codes, dn_scales, ig, gu, gd,
    xs, xr, xo, wf, wn, wb, wide, hid, act, hs, hr, g, r,
    x_send, x_recv, w_send, w_recv, a_send, a_recv, h_send, h_recv, r_send, r_recv,
):
    node, loc = lax.axis_index("node"), lax.axis_index("local")
    tokens, depth = tok.shape
    hidden = up_codes.shape[1]
    up, dn = wn.at[0], wn.at[1]
    rows = depth // n_local
    owned = rows // n_node
    bits = n_node.bit_length() - 1
    parts = 2 if paired_rows else 1
    others = range(1, n_local)
    halves = hidden // QBLOCK
    piece = tokens // pieces

    def target(step):
        return lax.rem(loc + step, n_local)

    def source(step):
        return lax.rem(loc + n_local - step, n_local)

    def columns(index):
        return pl.ds(pl.multiple_of(index * rows, 128), rows)

    barrier = pltpu.get_barrier_semaphore()
    for step in others:
        pl.semaphore_signal(barrier, inc=1, device_id={"local": target(step)}, device_id_type=MESH)
    for bit in range(bits):
        pl.semaphore_signal(barrier, inc=1, device_id={"node": flipped(node, bit)}, device_id_type=MESH)
    pl.semaphore_wait(barrier, n_local - 1 + bits)

    far = [bit for bit in range(bits - 1, -1, -1)]
    near = [1] + [bit for bit in range(bits - 1, 1, -1)] + [0] if bits > 1 else far
    gather_orders = (far, near)

    def stage_columns(values, m, index, store):
        if not paired_rows:
            store(0, slice(0, rows), values[:, columns(index)].astype(F32))
            return
        for pair in range(n_node // 2):
            begin = index * rows + pair * 2 * owned
            both = values[:, pl.ds(pl.multiple_of(begin, 128), 2 * owned)].astype(F32)
            cut = slice(pair * owned, (pair + 1) * owned)
            for part, tile in enumerate(paired(both[:, :owned], both[:, owned:])):
                store(part, cut, tile)

    x_copies = {}
    for m in range(2):
        for step in others:
            for part in range(parts):
                for c in range(pieces):
                    x_copies[m, step, part, c] = pltpu.make_async_remote_copy(
                        src_ref=xs.at[step - 1, m, part, pl.ds(c * piece, piece)],
                        dst_ref=xr.at[step - 1, m, part, pl.ds(c * piece, piece)],
                        send_sem=x_send.at[step - 1, m, part, c],
                        recv_sem=x_recv.at[step - 1, m, part, c],
                        device_id={"local": target(step)},
                        device_id_type=MESH,
                    )

    def send_columns(m, part, c):
        for step in others:
            x_copies[m, step, part, c].start()

    def stage_sends(m):
        for step in others:

            def store(part, cut, tile):
                xs[step - 1, m, part, :, cut] = tile

            stage_columns((tok, og)[m], m, target(step), store)

    stage_sends(0)
    send_columns(0, 0, 0)

    for m, (codes, scales) in enumerate(((up_codes, up_scales), (dn_codes, dn_scales))):
        for begin in range(0, rows, QBLOCK):
            down_cut = slice(begin, begin + QBLOCK)
            for f in range(halves):
                lanes = slice(f * QBLOCK, (f + 1) * QBLOCK)
                wide_scales = jnp.broadcast_to(scales[f : f + 1, down_cut], (QBLOCK, QBLOCK)).T
                value = (codes[down_cut, lanes].astype(F32) * wide_scales).astype(BF16)
                wn[m, down_cut, lanes] = value
                wf[m, down_cut, lanes] = value.astype(F32)

    w_copies = {}
    for m in range(2):
        for step in others:
            w_copies[m, step] = pltpu.make_async_remote_copy(
                src_ref=wf.at[m, pl.ds(pl.multiple_of(node * owned, 8), owned)],
                dst_ref=wb.at[step - 1, m, place(node, gather_orders[m])],
                send_sem=w_send.at[step - 1, m],
                recv_sem=w_recv.at[step - 1, m],
                device_id={"local": target(step)},
                device_id_type=MESH,
            )
            w_copies[m, step].start()

    queue = [(m, part, c) for m in range(2) for part in range(parts) for c in range(pieces)][1:]
    early = 2 * len(queue) // 3
    for m, part, c in queue[:early]:
        if m == 0:
            send_columns(m, part, c)
    stage_sends(1)
    for m, part, c in queue[:early]:
        if m == 1:
            send_columns(m, part, c)
    if paired_rows:
        for m in range(2):

            def keep(part, cut, tile):
                xo[m, part, :, cut] = tile.astype(BF16)

            stage_columns((tok, og)[m], m, loc, keep)

    sums = [
        jnp.dot(tok[:, columns(loc)], up[...], preferred_element_type=F32),
        jnp.dot(og[:, columns(loc)], dn[...], preferred_element_type=F32),
    ]

    a_copies = {}
    for stage in range(bits):
        for m in range(2):
            for step in others:
                if stage == 0:
                    w_copies[m, step].wait_recv()
                else:
                    a_copies[m, step, stage - 1].wait_recv()
                size = 1 << stage
                at = place(node, gather_orders[m])
                held = wb.at[step - 1, m, pl.ds((at // size) * size, size)]
                a_copies[m, step, stage] = pltpu.make_async_remote_copy(
                    src_ref=held,
                    dst_ref=held,
                    send_sem=a_send.at[step - 1, m, stage],
                    recv_sem=a_recv.at[step - 1, m, stage],
                    device_id={"node": flipped(node, gather_orders[m][stage])},
                    device_id_type=MESH,
                )
                a_copies[m, step, stage].start()
    for m in range(2):
        for step in others:
            a_copies[m, step, bits - 1].wait_recv()
            for n in range(n_node):
                wide[step - 1, m, n * owned : (n + 1) * owned, :] = wb[
                    step - 1, m, place(n, gather_orders[m])
                ].astype(BF16)
            sums[m] += jnp.dot(
                (tok, og)[m][:, columns(source(step))],
                wide[step - 1, m],
                preferred_element_type=F32,
            )

    pre, back = sums
    root = 0.7978845608028654
    square = pre * pre
    bend = jnp.tanh(root * (pre + 0.044715 * (square * pre)))
    half = 0.5 * (1.0 + bend)
    slope = half + 0.5 * pre * (1.0 - bend * bend) * (root * (1.0 + 3.0 * 0.044715 * square))
    act[...] = (half * pre).astype(BF16)
    hid[...] = (back * slope).astype(BF16)
    hs[0] = hid[...].astype(F32)
    hs[1] = act[...].astype(F32)
    h_copies = {}
    for m in range(2):
        for step in others:
            h_copies[m, step] = pltpu.make_async_remote_copy(
                src_ref=hs.at[m],
                dst_ref=hr.at[step - 1, m],
                send_sem=h_send.at[step - 1, m],
                recv_sem=h_recv.at[step - 1, m],
                device_id={"local": target(step)},
                device_id_type=MESH,
            )
            h_copies[m, step].start()
    for m, part, c in queue[early:]:
        send_columns(m, part, c)

    across = (((1,), (1,)), ((), ()))
    ig[:, columns(loc)] = lax.dot_general(
        hid[...], up[...], across, preferred_element_type=F32
    ).astype(BF16)
    for step in others:
        ig[:, columns(source(step))] = lax.dot_general(
            hid[...], wide[step - 1, 0], across, preferred_element_type=F32
        ).astype(BF16)

    chunks = [(m, f) for m in range(2) for f in range(2 if paired_rows else halves)]
    units = parts
    add_orders = [gather_orders[u % 2] for u in range(units * len(chunks))]
    height = g.shape[2]
    down_rows = (((0,), (0,)), ((), ()))
    axis = 0 if paired_rows else 1
    width = rows // parts
    block = min(width, 256)

    def term(features, values):
        pair = (features, values) if paired_rows else (values, features)
        return coded(lax.dot_general(*pair, down_rows, preferred_element_type=F32), axis)

    def compute(k):
        m, f = chunks[k]
        part = f if paired_rows else 0
        for step in others:
            if f == 0:
                h_copies[m, step].wait_recv()
            if paired_rows or f == 0:
                for c in range(pieces):
                    x_copies[m, step, part, c].wait_recv()
        for start in range(0, width, block):
            cut = slice(start, start + block)
            if paired_rows:
                own = xo[m, part, :, cut]
            else:
                own = (tok, og)[m][:, pl.ds(pl.multiple_of(loc * rows + start, 128), block)]
            received = [xr[step - 1, m, part, :, cut].astype(BF16) for step in others]
            totals = []
            for at in range(halves) if paired_rows else (f,):
                lanes = slice(at * QBLOCK, (at + 1) * QBLOCK)
                total = term((hid, act)[m][:, lanes], own)
                for step in others:
                    total += term(hr[step - 1, m, :, lanes].astype(BF16), received[step - 1])
                totals.append(coded(total, axis))
            if paired_rows:
                for tile in range(block // QBLOCK):
                    lanes = slice(tile * QBLOCK, (tile + 1) * QBLOCK)
                    owner = 2 * (start // QBLOCK + tile)
                    for sub, value in enumerate(paired(totals[0][:, lanes], totals[1][:, lanes])):
                        for u in range(units):
                            at = place(owner + sub, add_orders[k * units + u])
                            g[k * units + u, at] = value[u * height : (u + 1) * height]
            else:
                for sub in range(block // owned):
                    at = place(start // owned + sub, add_orders[k])
                    g[k, at] = totals[0][sub * owned : (sub + 1) * owned, :]

    region = [0] * len(add_orders)
    r_copies = {}

    def start(k, stage):
        bit = add_orders[k][bits - 1 - stage]
        size = n_node >> (stage + 1)
        mine = (node // (1 << bit)) % 2
        r_copies[k, stage] = pltpu.make_async_remote_copy(
            src_ref=g.at[k, pl.ds(region[k] + (1 - mine) * size, size)],
            dst_ref=r.at[k, pl.ds(n_node - 2 * size, size)],
            send_sem=r_send.at[k, stage],
            recv_sem=r_recv.at[k, stage],
            device_id={"node": flipped(node, bit)},
            device_id_type=MESH,
        )
        r_copies[k, stage].start()
        region[k] = region[k] + mine * size

    def finish(k, stage):
        size = n_node >> (stage + 1)
        r_copies[k, stage].wait_recv()

        def add(i, carry):
            g[k, region[k] + i] += r[k, n_node - 2 * size + i]
            return carry

        lax.fori_loop(0, size, add, 0)

    def emit(k):
        m, f = chunks[k]
        value = jnp.concatenate(
            [g[u, region[u]] for u in range(k * units, (k + 1) * units)], axis=0
        ) * (1.0 / (n_node * n_local))
        if paired_rows:
            turned = value.T
            size = owned // 2
            for at in range(2):
                (gu, gd)[m][f * size : (f + 1) * size, at * QBLOCK : (at + 1) * QBLOCK] = turned[
                    at * size : (at + 1) * size
                ]
        else:
            (gu, gd)[m][:, f * QBLOCK : (f + 1) * QBLOCK] = value

    begins = [0.0, 0.4, 2.6, 7.6] if len(chunks) == 4 else list(range(len(chunks)))
    events = sorted(
        (begins[k] + stage, k, stage) for k in range(len(chunks)) for stage in range(bits + 1)
    )
    for _, k, stage in events:
        if stage == 0:
            compute(k)
        for u in range(k * units, (k + 1) * units):
            if stage > 0:
                finish(u, stage - 1)
            if stage < bits:
                start(u, stage)
        if stage == bits:
            emit(k)

    for copies in (w_copies, x_copies, a_copies, h_copies, r_copies):
        for copy in copies.values():
            copy.wait_send()


def local(n_node, n_local, tokens, out_grad, up_codes, up_scales, down_codes, down_scales):
    count, depth = tokens.shape
    rows, hidden = up_codes.shape
    owned = rows // n_node
    bits = n_node.bit_length() - 1
    pieces = 4 if count % 32 == 0 else 1
    paired_rows = owned == QBLOCK and hidden == 2 * QBLOCK and n_node % 2 == 0
    parts = 2 if paired_rows else 1
    chunks = 4 if paired_rows else 2 * (hidden // QBLOCK)
    others = n_local - 1
    units = parts
    block = (owned // units, QBLOCK)
    dma = pltpu.SemaphoreType.DMA
    vmem = pl.BlockSpec(memory_space=pltpu.VMEM)
    return pl.pallas_call(
        functools.partial(kernel, n_node, n_local, paired_rows, pieces),
        out_shape=(
            jax.ShapeDtypeStruct((count, depth), BF16),
            jax.ShapeDtypeStruct((owned, hidden), F32),
            jax.ShapeDtypeStruct((owned, hidden), F32),
        ),
        in_specs=[vmem] * 6,
        out_specs=(vmem, vmem, vmem),
        scratch_shapes=[
            pltpu.VMEM((others, 2, parts, count, rows // parts), F32),
            pltpu.VMEM((others, 2, parts, count, rows // parts), F32),
            pltpu.VMEM((2, parts, count, rows // parts), BF16),
            pltpu.VMEM((2, rows, hidden), F32),
            pltpu.VMEM((2, rows, hidden), BF16),
            pltpu.VMEM((others, 2, n_node, owned, hidden), F32),
            pltpu.VMEM((others, 2, rows, hidden), BF16),
            pltpu.VMEM((count, hidden), BF16),
            pltpu.VMEM((count, hidden), BF16),
            pltpu.VMEM((2, count, hidden), F32),
            pltpu.VMEM((others, 2, count, hidden), F32),
            pltpu.VMEM((chunks * units, n_node) + block, F32),
            pltpu.VMEM((chunks * units, n_node) + block, F32),
            dma((others, 2, parts, pieces)),
            dma((others, 2, parts, pieces)),
            dma((others, 2)),
            dma((others, 2)),
            dma((others, 2, bits)),
            dma((others, 2, bits)),
            dma((others, 2)),
            dma((others, 2)),
            dma((chunks * units, bits)),
            dma((chunks * units, bits)),
        ],
        compiler_params=pltpu.CompilerParams(
            collective_id=0, has_side_effects=True, vmem_limit_bytes=56 * 1024 * 1024
        ),
    )(tokens, out_grad, up_codes, up_scales.T, down_codes, down_scales.T)


def solution(mesh):
    placed = (
        P(("node", "local"), None),
        P(("node", "local"), None),
        P("local", None),
        P("local", None),
        P("local", None),
        P("local", None),
    )
    return jax.shard_map(
        functools.partial(local, mesh.shape["node"], mesh.shape["local"]),
        mesh=mesh,
        in_specs=placed,
        out_specs=(
            P(("node", "local"), None),
            P(("local", "node"), None),
            P(("local", "node"), None),
        ),
        check_vma=False,
    )
```
